8 devices in a mesh: dp: 1 (over z), embed: 2 (over y), heads: 4 (over x, core).
Axes of the slice: x: 2, y: 2, z: 1, core: 2. Of those that a mesh axis runs over, the one named last changes fastest.
Arguments:
- x_in: bfloat16 [8192, 2048], P('dp', 'embed')
- positions: int32 [256], P('dp')
- gain_one: float32 [2048], P('embed')
- gain_two: float32 [2048], P('embed')
- w_qkv: bfloat16 [2048, 8, 384], P('embed', 'heads')
- w_out: bfloat16 [2048, 2048], P('heads', 'embed')
- w_gu: bfloat16 [2048, 2, 8192], P('embed', None, 'heads')
- w_down: bfloat16 [8192, 2048], P('heads', 'embed')
- grad_out: bfloat16 [8192, 2048], P('dp', 'embed')
Outputs:
- output 1: bfloat16 [8192, 2048], P('dp', 'embed')
- output 2: bfloat16 [8192, 2048], P('dp', 'embed')
- output 3: float32 [2048], P(('dp', 'embed'))
- output 4: float32 [2048], P(('dp', 'embed'))
- output 5: float32 [2048, 8, 384], P(('dp', 'embed'), 'heads')
- output 6: float32 [2048, 2048], P(('dp', 'heads'), 'embed')
- output 7: float32 [2048, 2, 8192], P(('dp', 'embed'), None, 'heads')
- output 8: float32 [8192, 2048], P(('dp', 'heads'), 'embed')
All inputs are finite; a program needn't handle non-finite values.
Results may differ from the reference program's by a relative error of at most 0.02.
Values are sent between devices in bfloat16 or wider.
A program may use at most 1 GiB of HBM per device.

```python
import jax
import jax.numpy as jnp
from jax import lax

D_MODEL = 2048
N_HEADS = 32
KV_HEADS = 8
HEAD_DIM = 64
FF_DIM = 8192
SEQ_LEN = 256
BATCH = 32

Q_PER_KV = N_HEADS // KV_HEADS
QKV_WIDTH = (Q_PER_KV + 2) * HEAD_DIM
TOKENS = BATCH * SEQ_LEN
EPSILON = 1e-5
ROPE_BASE = 10000.0
TWO_PI = 6.283185307179586


def setup_inputs(seed: int = 0, part: int = 0) -> dict:
    part_keys = jax.random.split(jax.random.fold_in(jax.random.key(seed), part), 5)
    shared_keys = jax.random.split(jax.random.key(seed + 1), 6)
    base_noise = jax.random.normal(part_keys[0], (TOKENS, D_MODEL), jnp.float32)
    token_phase = jax.random.uniform(part_keys[1], (TOKENS, 1), jnp.float32) * TWO_PI
    col_angle = TWO_PI * jnp.arange(D_MODEL, dtype=jnp.float32)[None, :] / D_MODEL
    x_in = (base_noise * jnp.exp(jnp.cos(col_angle - token_phase))).astype(jnp.bfloat16)
    pos_gaps = jax.random.randint(part_keys[2], (SEQ_LEN,), 1, 4)
    offset = jax.random.randint(part_keys[3], (1,), 0, 1024)
    positions = (offset + jnp.cumsum(pos_gaps)).astype(jnp.int32)
    grad_out = jax.random.normal(part_keys[4], (TOKENS, D_MODEL), jnp.float32).astype(jnp.bfloat16)
    gain_one = 1.0 + 0.3 * jax.random.normal(shared_keys[0], (D_MODEL,), jnp.float32)
    gain_two = 1.0 + 0.3 * jax.random.normal(shared_keys[1], (D_MODEL,), jnp.float32)
    w_qkv = (jax.random.normal(shared_keys[2], (D_MODEL, KV_HEADS, QKV_WIDTH), jnp.float32) * D_MODEL ** -0.5).astype(jnp.bfloat16)
    w_out = (jax.random.normal(shared_keys[3], (N_HEADS * HEAD_DIM, D_MODEL), jnp.float32) * (N_HEADS * HEAD_DIM) ** -0.5).astype(jnp.bfloat16)
    w_gu = (jax.random.normal(shared_keys[4], (D_MODEL, 2, FF_DIM), jnp.float32) * D_MODEL ** -0.5).astype(jnp.bfloat16)
    w_down = (jax.random.normal(shared_keys[5], (FF_DIM, D_MODEL), jnp.float32) * FF_DIM ** -0.5).astype(jnp.bfloat16)
    return {'x_in': x_in, 'positions': positions, 'gain_one': gain_one, 'gain_two': gain_two, 'w_qkv': w_qkv, 'w_out': w_out, 'w_gu': w_gu, 'w_down': w_down, 'grad_out': grad_out}


def as_bf16(operand):
    return operand.astype(jnp.bfloat16).astype(jnp.float32)


def rope_tables(positions):
    inv_freq = ROPE_BASE ** (-jnp.arange(0, HEAD_DIM, 2, dtype=jnp.float32) / HEAD_DIM)
    angles = positions.astype(jnp.float32)[:, None] * inv_freq[None, :]
    angles = jnp.concatenate([angles, angles], axis=-1)
    return jnp.cos(angles), jnp.sin(angles)


def apply_rope(operand, cos_t, sin_t):
    half_dim = HEAD_DIM // 2
    rotated = jnp.concatenate([-operand[..., half_dim:], operand[..., :half_dim]], axis=-1)
    return as_bf16(operand * cos_t + rotated * sin_t)


def rms_norm(hidden, gain):
    inv_rms = lax.rsqrt(jnp.mean(hidden * hidden, axis=-1, keepdims=True) + EPSILON)
    return as_bf16(hidden * inv_rms * gain)


def group_attention(group_qkv, cos_t, sin_t):
    q_cut = Q_PER_KV * HEAD_DIM
    queries = group_qkv[..., :q_cut].reshape(BATCH, SEQ_LEN, Q_PER_KV, HEAD_DIM).transpose(0, 2, 1, 3)
    queries = apply_rope(queries, cos_t, sin_t)
    key_rot = apply_rope(group_qkv[..., q_cut:q_cut + HEAD_DIM], cos_t, sin_t)
    values = group_qkv[..., q_cut + HEAD_DIM:]
    scores = jnp.einsum('bgqh,bsh->bgqs', queries, key_rot) * HEAD_DIM ** -0.5
    causal = jnp.arange(SEQ_LEN)[:, None] >= jnp.arange(SEQ_LEN)[None, :]
    attn_probs = as_bf16(jax.nn.softmax(jnp.where(causal, scores, -1e30), axis=-1))
    attn_mix = as_bf16(jnp.einsum('bgqs,bsh->bqgh', attn_probs, values))
    return attn_mix.reshape(BATCH, SEQ_LEN, q_cut)


def reference(x_in, positions, gain_one, gain_two, w_qkv, w_out, w_gu, w_down, grad_out):
    cos_t, sin_t = rope_tables(positions)

    def forward(x_val, gain_a, gain_b, qkv_w, out_w, gu_w, down_w):
        normed = rms_norm(x_val, gain_a)
        qkv_all = as_bf16(jnp.einsum('td,dgc->tgc', normed, qkv_w))
        qkv_all = qkv_all.reshape(BATCH, SEQ_LEN, KV_HEADS, QKV_WIDTH).transpose(2, 0, 1, 3)
        attn_mix = lax.map(jax.checkpoint(lambda group_qkv: group_attention(group_qkv, cos_t, sin_t)), qkv_all)
        attn_mix = attn_mix.transpose(1, 2, 0, 3).reshape(TOKENS, N_HEADS * HEAD_DIM)
        hidden = as_bf16(x_val + as_bf16(jnp.dot(attn_mix, out_w, preferred_element_type=jnp.float32)))
        normed_two = rms_norm(hidden, gain_b)
        gate_up = as_bf16(jnp.einsum('td,dkf->tkf', normed_two, gu_w))
        act_out = as_bf16(jax.nn.silu(gate_up[:, 0]) * gate_up[:, 1])
        return as_bf16(hidden + as_bf16(jnp.dot(act_out, down_w, preferred_element_type=jnp.float32)))

    y_val, pullback = jax.vjp(forward, x_in.astype(jnp.float32), gain_one, gain_two, w_qkv.astype(jnp.float32), w_out.astype(jnp.float32), w_gu.astype(jnp.float32), w_down.astype(jnp.float32))
    grads = pullback(grad_out.astype(jnp.float32))
    return (y_val.astype(jnp.bfloat16), grads[0].astype(jnp.bfloat16), grads[1], grads[2], grads[3], grads[4], grads[5], grads[6])
```

```python
import functools

import jax
import jax.numpy as jnp
from jax import lax
from jax.experimental import pallas as pl
from jax.experimental.pallas import tpu as pltpu
from jax.sharding import PartitionSpec as P

EPSILON = 1e-5
ROPE_BASE = 10000.0
F32 = jnp.float32
BF16 = jnp.bfloat16


NN = (((1,), (0,)), ((), ()))
NT = (((1,), (1,)), ((), ()))
TN = (((0,), (0,)), ((), ()))


def mm(lhs, rhs, dims=NN):
    return lax.dot_general(lhs, rhs, dims, preferred_element_type=F32)


def rope_tables(positions, head_dim):
    inv_freq = ROPE_BASE ** (-jnp.arange(0, head_dim, 2, dtype=F32) / head_dim)
    angles = positions.astype(F32)[:, None] * inv_freq[None, :]
    cos_h, sin_h = jnp.cos(angles), jnp.sin(angles)
    return jnp.concatenate([cos_h] * 4, axis=-1), jnp.concatenate([-sin_h, sin_h] * 2, axis=-1)


def lane_masks(seq_len):
    lane = lax.broadcasted_iota(jnp.int32, (seq_len, 128), 1)
    return (lane % 64) < 32, lane < 64


def swap_halves(tile, low):
    return jnp.where(low, pltpu.roll(tile, 96, 1), pltpu.roll(tile, 32, 1))


def causal_transposed(seq_len):
    key = lax.broadcasted_iota(jnp.int32, (seq_len, seq_len), 0)
    query = lax.broadcasted_iota(jnp.int32, (seq_len, seq_len), 1)
    return key <= query


def probs_transposed(key_tile, query_tile, causal):
    scores = jnp.where(causal, mm(key_tile, query_tile, NT), -1e30)
    top = jnp.max(scores, axis=0, keepdims=True)
    weights = jnp.exp(scores - top)
    return weights * (1.0 / jnp.sum(weights, axis=0, keepdims=True))


def attn_fwd_kernel(qkv_ref, cos_ref, sin_ref, out_ref):
    seq_len = qkv_ref.shape[0]
    low, first = lane_masks(seq_len)
    causal = causal_transposed(seq_len)
    cos_t, sin_t = cos_ref[...], sin_ref[...]
    kv = qkv_ref[:, 256:384].astype(F32)
    key = jnp.where(first, kv * cos_t + swap_halves(kv, low) * sin_t, 0.0)
    keys = (key.astype(BF16), pltpu.roll(key, 64, 1).astype(BF16))
    val_t = kv.T[64:128, :].astype(BF16)
    cos_q, sin_q = cos_t * 0.125, sin_t * 0.125
    mixes = []
    for tile in range(2):
        query = qkv_ref[:, 128 * tile:128 * tile + 128].astype(F32)
        query = (query * cos_q + swap_halves(query, low) * sin_q).astype(BF16)
        for half in range(2):
            probs = probs_transposed(keys[half], query, causal).astype(BF16)
            mixes.append(mm(val_t, probs))
    out_ref[...] = jnp.concatenate(mixes, axis=0).T.astype(BF16)


def attn_bwd_kernel(qkv_ref, grad_ref, cos_ref, sin_ref, out_ref):
    seq_len = qkv_ref.shape[0]
    low, first = lane_masks(seq_len)
    causal = causal_transposed(seq_len)
    cos_t, sin_t = cos_ref[...], sin_ref[...]
    kv = qkv_ref[:, 256:384].astype(F32)
    key = jnp.where(first, kv * cos_t + swap_halves(kv, low) * sin_t, 0.0)
    keys = (key.astype(BF16), pltpu.roll(key, 64, 1).astype(BF16))
    key_t = key.T[0:64, :].astype(BF16)
    val = jnp.where(first, 0.0, kv)
    vals = (pltpu.roll(val, 64, 1).astype(BF16), val.astype(BF16))
    cos_q, sin_q = cos_t * 0.125, sin_t * 0.125
    grad_key = jnp.zeros((seq_len, 128), F32)
    grad_val = jnp.zeros((seq_len, 128), F32)
    grad_queries = []
    for tile in range(2):
        query = qkv_ref[:, 128 * tile:128 * tile + 128].astype(F32)
        query = query * cos_q + swap_halves(query, low) * sin_q
        grad = grad_ref[:, 128 * tile:128 * tile + 128]
        grad32 = grad.astype(F32)
        query_b = query.astype(BF16)
        for half in range(2):
            mine = first if half == 0 else jnp.logical_not(first)
            query_m = jnp.where(mine, query, 0.0).astype(BF16)
            grad_m = jnp.where(mine, grad32, 0.0).astype(BF16)
            probs = probs_transposed(keys[half], query_b, causal)
            grad_p = mm(vals[half], grad, NT).astype(BF16).astype(F32)
            dots = jnp.sum(probs * grad_p, axis=0, keepdims=True)
            grad_s = (probs * (grad_p - dots)).astype(BF16)
            grad_val = grad_val + mm(probs.astype(BF16), grad_m)
            grad_key = grad_key + mm(grad_s, query_m)
            grad_queries.append(mm(key_t, grad_s))
    grad_q = (jnp.concatenate(grad_queries, axis=0).T * 0.125).astype(BF16).astype(F32)
    for tile in range(2):
        part = grad_q[:, 128 * tile:128 * tile + 128]
        out_ref[:, 128 * tile:128 * tile + 128] = (part * cos_t + swap_halves(part * sin_t, low)).astype(BF16)
    grad_key = (grad_key + pltpu.roll(grad_key, 64, 1)).astype(BF16).astype(F32)
    grad_key = grad_key * cos_t + swap_halves(grad_key * sin_t, low)
    grad_val = grad_val + pltpu.roll(grad_val, 64, 1)
    out_ref[:, 256:384] = jnp.where(first, grad_key, grad_val).astype(BF16)


def attention(qkv, cos_t, sin_t, grad=None):
    seq_len = cos_t.shape[0]
    tokens, width = qkv.shape
    groups, seqs = width // 384, tokens // seq_len
    table = pl.BlockSpec((seq_len, 128), lambda s, g: (0, 0))
    wide = pl.BlockSpec((seq_len, 384), lambda s, g: (s, g))
    narrow = pl.BlockSpec((seq_len, 256), lambda s, g: (s, g))
    heads = seqs * groups * 4
    if grad is None:
        return pl.pallas_call(
            attn_fwd_kernel,
            out_shape=jax.ShapeDtypeStruct((tokens, groups * 256), BF16),
            grid=(seqs, groups),
            in_specs=[wide, table, table],
            out_specs=narrow,
            cost_estimate=pl.CostEstimate(flops=heads * 150_000_000, bytes_accessed=tokens * groups * 1280, transcendentals=0),
            name="attn_fwd",
        )(qkv, cos_t, sin_t)
    return pl.pallas_call(
        attn_bwd_kernel,
        out_shape=jax.ShapeDtypeStruct((tokens, groups * 384), BF16),
        grid=(seqs, groups),
        in_specs=[wide, narrow, table, table],
        out_specs=wide,
        cost_estimate=pl.CostEstimate(flops=heads * 350_000_000, bytes_accessed=tokens * groups * 2048, transcendentals=0),
        name="attn_bwd",
    )(qkv, grad, cos_t, sin_t)


def rms_forward(hidden, gain):
    hidden32 = hidden.astype(F32)
    inv_rms = lax.rsqrt(jnp.mean(hidden32 * hidden32, axis=-1, keepdims=True) + EPSILON)
    return (hidden32 * inv_rms * gain).astype(BF16), inv_rms


def rms_backward(grad_normed, hidden, inv_rms, gain):
    grad_in = grad_normed.astype(F32)
    unit_rows = hidden.astype(F32) * inv_rms
    grad_gain = jnp.sum(grad_in * unit_rows, axis=0)
    scaled = grad_in * gain
    dots = jnp.mean(scaled * unit_rows, axis=-1, keepdims=True)
    return inv_rms * (scaled - unit_rows * dots), grad_gain


def solution(mesh):
    embed_size, heads_size = mesh.shape['embed'], mesh.shape['heads']
    assert embed_size == 2 and heads_size == 4 and mesh.shape['dp'] == 1

    def swap_y(value):
        return lax.ppermute(value, 'embed', [(0, 1), (1, 0)])

    def swap_c(value):
        return lax.ppermute(value, 'heads', [(i, i ^ 1) for i in range(4)])

    def swap_x(value):
        return lax.ppermute(value, 'heads', [(i, i ^ 2) for i in range(4)])

    def per_device(x_in, positions, gain_one, gain_two, w_qkv, w_out, w_gu, w_down, grad_out):
        e_idx, h_idx = lax.axis_index('embed'), lax.axis_index('heads')
        tokens, half = x_in.shape
        rows = tokens // 8
        width = 2 * half
        groups, qkv_width = w_qkv.shape[1], w_qkv.shape[2]
        head_dim = 64
        cols = groups * qkv_width
        mix = w_out.shape[0]
        ff = w_gu.shape[2]

        def block_of(array, h_pos, e_pos):
            return lax.dynamic_slice_in_dim(array, (2 * h_pos + e_pos) * rows, rows, 0)

        wq_mine = w_qkv.reshape(half, cols)
        wq_oth = swap_y(wq_mine)
        x_oth = swap_y(block_of(x_in, h_idx, 1 - e_idx))
        gains_mine = jnp.stack([gain_one, gain_two])
        gains = jnp.concatenate([gains_mine, swap_y(gains_mine)], axis=1)
        wo_oth = swap_y(w_out)
        wgu_oth = swap_y(w_gu)
        dy_oth = swap_y(block_of(grad_out, h_idx, 1 - e_idx))
        wd_oth = swap_y(w_down)

        cos_t, sin_t = rope_tables(positions, head_dim)

        wq0 = jnp.concatenate([wq_mine, wq_oth], axis=0)
        wq2 = swap_x(wq0)
        wq1 = swap_c(wq0)
        wq3 = swap_c(wq2)
        wq = [wq0, wq2, wq1, wq3]
        wo0 = jnp.concatenate([w_out, wo_oth], axis=1)
        wo2 = swap_x(wo0)
        wo1 = swap_c(wo0)
        wo3 = swap_c(wo2)
        wo = [wo0, wo2, wo1, wo3]

        x_own = jnp.concatenate([block_of(x_in, h_idx, e_idx), x_oth], axis=1)
        normed_one, inv_one = rms_forward(x_own, gains[0])
        qkv = [mm(normed_one, piece).astype(BF16) for piece in wq]
        mixes = [attention(piece, cos_t, sin_t) for piece in qkv]
        mix_all = jnp.concatenate(mixes, axis=1)
        wo_all = jnp.concatenate(wo, axis=0)
        attn_out = mm(mix_all, wo_all).astype(BF16)
        hidden = (x_own.astype(F32) + attn_out.astype(F32)).astype(BF16)
        normed_two, inv_two = rms_forward(hidden, gains[1])

        n2_x = swap_x(normed_two)
        n2_c = swap_c(normed_two)
        n2_xc = swap_c(n2_x)
        n2_all = jnp.concatenate([normed_two, n2_x, n2_c, n2_xc], axis=0)
        w_gate = jnp.concatenate([w_gu[:, 0, :], wgu_oth[:, 0, :]], axis=0)
        w_up = jnp.concatenate([w_gu[:, 1, :], wgu_oth[:, 1, :]], axis=0)
        w_gup = jnp.concatenate([w_gate, w_up], axis=1)
        gate_up = mm(n2_all, w_gup).astype(BF16)
        gate, up = gate_up[:, :ff].astype(F32), gate_up[:, ff:].astype(F32)
        sig = jax.nn.sigmoid(gate)
        act = (gate * sig * up).astype(BF16)

        dy_x = swap_x(dy_oth)
        dy_c = swap_c(dy_oth)
        dy_xc = swap_c(dy_x)
        dy_mine = [block_of(grad_out, h_idx ^ k, e_idx) for k in (0, 2, 1, 3)]
        dy_all = jnp.concatenate([jnp.concatenate(dy_mine, axis=0), jnp.concatenate([dy_oth, dy_x, dy_c, dy_xc], axis=0)], axis=1)
        dy_own = jnp.concatenate([dy_mine[0], dy_oth], axis=1)
        wd_all = jnp.concatenate([w_down, wd_oth], axis=1)

        grad_act = mm(dy_all, wd_all, NT).astype(BF16).astype(F32)
        grad_up = (grad_act * (gate * sig)).astype(BF16)
        grad_gate = (grad_act * up * (sig * (1.0 + gate * (1.0 - sig)))).astype(BF16)
        grad_gu = jnp.concatenate([grad_gate, grad_up], axis=1)

        gwd_oth = swap_y(mm(act, dy_all[:, half:], TN).astype(BF16))
        grad_w_down = mm(act, dy_all[:, :half], TN) + gwd_oth.astype(F32)
        ggu_oth = swap_y(mm(n2_all[:, half:], grad_gu, TN).astype(BF16))
        grad_w_gup = mm(n2_all[:, :half], grad_gu, TN) + ggu_oth.astype(F32)
        grad_w_gu = jnp.stack([grad_w_gup[:, :ff], grad_w_gup[:, ff:]], axis=1)

        def sum_heads(lhs, rhs, dims):
            from_c = swap_c(mm(lhs[2 * rows:], rhs, dims).astype(BF16))
            keep = mm(lhs[:2 * rows], rhs, dims) + from_c.astype(F32)
            from_x = swap_x(keep[rows:].astype(BF16))
            return keep[:rows].astype(BF16).astype(F32) + from_x.astype(F32)

        grad_n2 = sum_heads(grad_gu, w_gup, NT).astype(BF16)
        mlp_out = sum_heads(act, wd_all, NN).astype(BF16)
        y_own = (hidden.astype(F32) + mlp_out.astype(F32)).astype(BF16)

        grad_h_norm, grad_gain_two = rms_backward(grad_n2, hidden, inv_two, gains[1])
        grad_hidden = (dy_own.astype(F32) + grad_h_norm).astype(BF16)

        grad_mix = [mm(grad_hidden, piece, NT).astype(BF16) for piece in wo]
        grad_qkv = [attention(piece, cos_t, sin_t, grad) for piece, grad in zip(qkv, grad_mix)]
        dqkv_all = jnp.concatenate(grad_qkv, axis=1)
        wq_all = jnp.concatenate(wq, axis=1)
        grad_n1 = mm(dqkv_all, wq_all, NT).astype(BF16)
        grad_x_norm, grad_gain_one = rms_backward(grad_n1, x_own, inv_one, gains[0])
        dx_own = (grad_hidden.astype(F32) + grad_x_norm).astype(BF16)

        go_c = swap_c(mm(mix_all[:, 2 * mix:], grad_hidden, TN).astype(BF16))
        go_x = swap_x((mm(mixes[1], grad_hidden, TN) + go_c[mix:].astype(F32)).astype(BF16))
        go_sum = go_c[:mix].astype(F32) + go_x.astype(F32)
        go_y = swap_y((mm(mixes[0], grad_hidden[:, half:], TN) + go_sum[:, half:]).astype(BF16))
        grad_w_out = mm(mixes[0], grad_hidden[:, :half], TN) + (go_sum[:, :half] + go_y.astype(F32))

        gq_c = swap_c(mm(normed_one, jnp.concatenate(grad_qkv[2:], axis=1), TN).astype(BF16))
        gq_x = swap_x((mm(normed_one, grad_qkv[1], TN) + gq_c[:, cols:].astype(F32)).astype(BF16))
        gq_sum = gq_c[:, :cols].astype(F32) + gq_x.astype(F32)
        gq_y = swap_y((mm(normed_one[:, half:], grad_qkv[0], TN) + gq_sum[half:]).astype(BF16))
        grad_wq = mm(normed_one[:, :half], grad_qkv[0], TN) + (gq_sum[:half] + gq_y.astype(F32))
        grad_w_qkv = grad_wq.reshape(half, groups, qkv_width)

        def spread(value):
            p00 = value[:, :half]
            p01 = swap_y(value[:, half:])
            p20, p21 = swap_x(p00), swap_x(p01)
            pieces = {(0, 0): p00, (0, 1): p01, (2, 0): p20, (2, 1): p21}
            for k in (0, 2):
                for j in (0, 1):
                    pieces[k ^ 1, j] = swap_c(pieces[k, j])
            out = jnp.zeros((tokens, half), BF16)
            for (k, j), piece in pieces.items():
                out = lax.dynamic_update_slice_in_dim(out, piece, (2 * (h_idx ^ k) + (e_idx ^ j)) * rows, 0)
            return out

        y_out = spread(y_own)
        grad_x = spread(dx_own)
        grad_gains = jnp.stack([grad_gain_one, grad_gain_two])
        first, second = grad_gains[:, :half], grad_gains[:, half:]
        natural = jnp.where(e_idx == 0, jnp.stack([first, second]), jnp.stack([second, first]))
        natural = lax.psum(natural, ('embed', 'heads'))
        gain_mine = lax.dynamic_index_in_dim(natural, e_idx, 0, keepdims=False)
        return (y_out, grad_x, gain_mine[0], gain_mine[1], grad_w_qkv, grad_w_out, grad_w_gu, grad_w_down)

    act_spec = P('dp', 'embed')
    in_specs = (act_spec, P('dp'), P('embed'), P('embed'), P('embed', 'heads', None), P('heads', 'embed'), P('embed', None, 'heads'), P('heads', 'embed'), act_spec)
    out_specs = (act_spec, act_spec, P(('dp', 'embed')), P(('dp', 'embed')), P(('dp', 'embed'), 'heads', None), P(('dp', 'heads'), 'embed'), P(('dp', 'embed'), None, 'heads'), P(('dp', 'heads'), 'embed'))
    return jax.shard_map(per_device, mesh=mesh, in_specs=in_specs, out_specs=out_specs, check_vma=False)
```
